32 devices in a mesh: league: 8 (over z, y), rep: 4 (over x, core).
Axes of the slice: x: 2, y: 2, z: 4, core: 2. Of those that a mesh axis runs over, the one named last changes fastest.
Arguments:
- observations: bfloat16 [4096, 2048], P(('league', 'rep')), may hold values from -6 to 6
- weights: bfloat16 [8, 2048, 2048], P('league', None, 'rep'), may hold values from -0.125 to 0.125
- gains: float32 [8, 2048], P('league'), may hold values from 0.5 to 1.5
- heads: bfloat16 [8, 2048], P('league', 'rep'), may hold values from -0.125 to 0.125
- pairing: int32 [4096, 1], P(('league', 'rep')), may hold values from 0 to 7; in each aligned block of 128 rows (0 to 127, 128 to 255, ...) at most 32 rows name the same one
- valid: int32 [4096], P(('league', 'rep')), may hold values 0 or 1
Outputs:
- own_value: float32 [4096], P(('league', 'rep'))
- opponent_value: float32 [4096], P(('league', 'rep'))
The draws below stay inside these ranges and needn't reach their ends.
Inputs may be any that keep to these rules, and one draw needn't show every extreme that they name: `pairing`: among the rows of one device, at most 32 name one agent; every agent is named by some row of the whole batch.
All inputs are finite; a program needn't handle non-finite values. No bound on the sum of `valid` on one device may be relied on, other than what follows from the above.
Results may differ from the reference program's by a relative error of at most 0.003.
Values may be sent and summed in bfloat16 or wider, within the bound.
A program may use at most 64 MiB of HBM per device.

```python
import math
import jax
import jax.numpy as jnp
import numpy as np
from jax import lax

D = 2048
R_DEV = 128
AGENTS = 8
CAP = 32
ROWS = 4096
N_LEAGUE = 8
N_REP = 4


def place_ends(values, own_key, smallest, largest):
    spot = [jax.random.randint(jax.random.fold_in(own_key, axis), (), 0, length) for axis, length in enumerate(values.shape)]
    main_axis = values.shape.index(max(values.shape))
    neighbour = spot[:main_axis] + [(spot[main_axis] + 1) % values.shape[main_axis]] + spot[main_axis + 1:]
    return values.at[tuple(spot)].set(smallest).at[tuple(neighbour)].set(largest)


def levels(rng, extent, shards, low, high):
    def one(position, blocks):
        heights = jax.random.uniform(jax.random.fold_in(jax.random.fold_in(rng, 6), position), (blocks,), jnp.float32, low / len(shards), high / len(shards))
        return jnp.repeat(jnp.exp(heights), extent[position] // blocks).reshape((-1,) + (1,) * (len(extent) - position - 1))

    gain = one(*shards[0])
    for cut in shards[1:]:
        gain = gain * one(*cut)
    return gain


def shared_out(stream_key, own, number, rows, amount, top, most, skew):
    sequence = jax.random.permutation(stream_key, amount)
    crowded, usual = load_shares(amount, rows * top, most, skew, True), load_shares(amount, rows * top, most, skew, False)
    places = jnp.arange(amount)

    def named(tallies, rotation):
        used = int((tallies > 0).sum())
        fixed = max(1, used // 4)
        shifted = fixed + (places - fixed + rotation * (used - fixed)) % max(1, amount - fixed)
        return jnp.zeros((amount,), jnp.int32).at[sequence[jnp.where(places < fixed, places, shifted)]].set(jnp.asarray(tallies, jnp.int32))

    tallies = jnp.where(number % 4 == 0, named(crowded, number // 4), named(usual, number - number // 4 - 1))
    mixed = jax.random.permutation(jax.random.fold_in(own, 3), amount)
    donor, receiver = mixed[0:amount // 2 * 2:2], mixed[1:amount // 2 * 2:2]
    margin = jnp.minimum(tallies[donor] - 1, most - tallies[receiver]) // 2
    margin = jnp.where((donor == sequence[0]) | (receiver == sequence[0]) | (tallies[receiver] == 0), 0, jnp.maximum(margin, 0))
    shifted = jax.random.randint(jax.random.fold_in(own, 4), (amount // 2,), 0, 1 << 20) % (margin + 1)
    tallies = tallies.at[donor].add(-shifted).at[receiver].add(shifted)
    labels = jnp.searchsorted(jnp.cumsum(tallies), jnp.arange(rows * top), side="right").astype(jnp.int32)
    grid = labels.reshape(top, rows).T
    grid = grid[jax.random.permutation(jax.random.fold_in(own, 1), rows)]
    rotation = jax.random.randint(jax.random.fold_in(own, 2), (rows, 1), 0, top)
    return jnp.take_along_axis(grid, (jnp.arange(top)[None, :] + rotation) % top, axis=1)


def load_shares(amount, total, most, slope, full):
    loads = [(1 << 20) // math.isqrt(standing ** slope) + 1 for standing in range(1, amount + 1)]
    largest = most if full else min(most, max(-(-total // amount), total * loads[0] // sum(loads)))
    least = 1 if total - largest >= amount - 1 else 0
    counts, rest = [largest] + [least] * (amount - 1), total - largest - least * (amount - 1)
    while rest > 0:
        free = [i for i in range(1, amount) if counts[i] < largest] or [i for i in range(1, amount) if counts[i] < most]
        whole, left = sum([loads[i] for i in free]), rest
        for i in free:
            more = min(most - counts[i], max(1, left * loads[i] // whole), rest)
            counts[i] = counts[i] + more
            rest = rest - more
    return np.array(counts)


def bell_draw(key, extent, deviation, reach, shards=(), kind=jnp.bfloat16):
    drawn = jax.random.normal(key, extent, jnp.float32) * deviation
    if len(shards) > 0:
        drawn = levels(key, extent, shards, -0.22, 0.18) * drawn
    return jnp.clip(drawn, min=-reach, max=reach).astype(kind)


def setup_inputs(seed: int = 0) -> dict:
    streams_of = jax.random.split(jax.random.key(seed), 7)
    observations = bell_draw(streams_of[0], (ROWS, D), 1.0, 6.0, ((0, 32),))
    weights = bell_draw(streams_of[1], (AGENTS, D, D), D ** -0.5, 0.125, ((0, 8), (2, 4)))
    gains = jnp.clip(1.0 + 0.1 * jax.random.normal(streams_of[2], (AGENTS, D), jnp.float32), 0.5, 1.5)
    heads = bell_draw(streams_of[3], (AGENTS, D), D ** -0.5, 0.125, ((0, 8), (1, 4)))
    pairing_keys = jax.random.split(jax.random.fold_in(streams_of[4], 1), ROWS // R_DEV)
    pairing_turns = jax.random.permutation(jax.random.fold_in(streams_of[4], 3), ROWS // R_DEV)
    pairing = jax.vmap(lambda own, number: shared_out(jax.random.fold_in(streams_of[4], 2), own, number, R_DEV, AGENTS, 1, CAP, 2))(pairing_keys, pairing_turns).reshape((ROWS, 1))
    valid = place_ends((jax.random.randint(streams_of[5], (ROWS,), 0, 4) < 3).astype(jnp.int32), jax.random.fold_in(streams_of[5], 1), 0, 1)
    return dict(observations=observations, weights=weights, gains=gains, heads=heads, pairing=pairing, valid=valid)


def normed_values(obs_rows, agent_gain, weight_cols, head_cols):
    wide_rows = obs_rows.astype(jnp.float32)
    squares = lax.optimization_barrier(jnp.mean(wide_rows * wide_rows, axis=1, keepdims=True))
    scaled = (wide_rows * lax.rsqrt(squares + 1e-06) * agent_gain).astype(jnp.bfloat16)
    hidden = jax.nn.silu(jnp.dot(scaled, weight_cols, preferred_element_type=jnp.float32))
    return lax.optimization_barrier(jnp.sum(hidden * head_cols.astype(jnp.float32), axis=1))

def own_block(inputs):
    block_rows, agent_gain, weight_full, head_full = inputs
    return normed_values(block_rows, agent_gain, weight_full, head_full)

def reference(observations, weights, gains, heads, pairing, valid):
    total_rows, feature_width = observations.shape
    per_agent = total_rows // AGENTS
    blocks = observations.reshape(AGENTS, per_agent, feature_width)
    own_value = lax.map(own_block, (blocks, gains, weights, heads)).reshape(total_rows)
    owner_id = pairing[:, 0].astype(jnp.int32)
    row_order = jnp.argsort(owner_id, stable=True).astype(jnp.int32)
    most_rows = N_LEAGUE * N_REP * CAP
    padded_order = jnp.concatenate([row_order, jnp.full((most_rows,), total_rows, jnp.int32)])
    padded_obs = jnp.concatenate([observations, jnp.zeros((1, feature_width), observations.dtype)])
    slot_iota = jnp.arange(most_rows, dtype=jnp.int32)

    def visit(collected, inputs):
        agent_id, agent_gain, weight_full, head_full = inputs
        first_row = jnp.sum((owner_id < agent_id).astype(jnp.int32)).astype(jnp.int32)
        row_count = jnp.sum((owner_id == agent_id).astype(jnp.int32)).astype(jnp.int32)
        row_index = lax.dynamic_slice_in_dim(padded_order, first_row, most_rows)
        row_values = normed_values(padded_obs[row_index], agent_gain, weight_full, head_full)
        target = jnp.where(slot_iota < row_count, row_index, total_rows)
        return (collected.at[target].set(row_values), None)
    agent_ids = jnp.arange(AGENTS, dtype=jnp.int32)
    collected, unused = lax.scan(visit, jnp.zeros((total_rows + 1,), jnp.float32), (agent_ids, gains, weights, heads))
    opponent_value = jnp.where(valid == 1, collected[:total_rows], jnp.zeros((total_rows,), jnp.float32))
    return (own_value, opponent_value)
```

```python
import functools

import jax
import jax.numpy as jnp
from jax import lax
from jax.experimental import pallas as pl
from jax.experimental.pallas import tpu as pltpu
from jax.sharding import PartitionSpec as P

MESH = pl.DeviceIdType.MESH
TILE = 512
PARTS = 4


def normed_values(obs_rows, agent_gain, weight_cols, head_cols):
    wide_rows = obs_rows.astype(jnp.float32)
    squares = jnp.mean(wide_rows * wide_rows, axis=1, keepdims=True)
    scaled = (wide_rows * lax.rsqrt(squares + 1e-06) * agent_gain).astype(jnp.bfloat16)
    hidden = jax.nn.silu(jnp.dot(scaled, weight_cols, preferred_element_type=jnp.float32))
    return jnp.sum(hidden * head_cols.astype(jnp.float32), axis=1)


def gathered_plan(observations, weights, gains, heads, pairing, valid):
    rows_dev, feature_width = observations.shape
    n_league = lax.axis_size("league")
    capacity = max(2, 2 * rows_dev // n_league)
    own_gain = gains[0]
    weight_full = lax.all_gather(weights[0], "rep", axis=1, tiled=True)
    head_full = lax.all_gather(heads[0], "rep", axis=0, tiled=True)
    own_value = normed_values(observations, own_gain, weight_full, head_full)
    owner_id = pairing[:, 0]
    is_live = valid == 1
    agent_iota = jnp.arange(n_league, dtype=jnp.int32)
    pick_table = ((owner_id[:, None] == agent_iota[None, :]) & is_live[:, None]).astype(jnp.float32)
    row_iota = jnp.arange(rows_dev, dtype=jnp.int32)
    earlier = (row_iota[:, None] > row_iota[None, :]).astype(jnp.float32)
    before = jnp.dot(earlier, pick_table, precision=lax.Precision.HIGHEST)
    slot_index = jnp.sum(before * pick_table, axis=1).astype(jnp.int32)
    target = jnp.where(is_live, owner_id * capacity + slot_index, n_league * capacity)
    outgoing = (
        jnp.zeros((n_league * capacity + 1, feature_width), jnp.bfloat16)
        .at[target]
        .set(observations)
    )
    outgoing = outgoing[: n_league * capacity].reshape(n_league, capacity, feature_width)
    received = lax.all_to_all(outgoing, "league", split_axis=0, concat_axis=0, tiled=True)
    flat_rows = received.reshape(received.shape[0] * received.shape[1], feature_width)
    answers = normed_values(flat_rows, own_gain, weight_full, head_full).reshape(
        received.shape[0], received.shape[1]
    )
    returned = lax.all_to_all(answers, "league", split_axis=0, concat_axis=0, tiled=True)
    flat_back = jnp.concatenate([returned.reshape(-1), jnp.zeros((1,), jnp.float32)])
    opponent_value = jnp.where(is_live, flat_back[target], 0.0)
    return (own_value, opponent_value)


def kernel(
    n, cap,
    obs_hbm, w_hbm, gain_hbm, head_hbm, pair_hbm, valid_hbm,
    out_ref,
    rows, wbuf, gain, head, pair, live, hv, code, slots, taken, distant, scaled, res, back, vown,
    lsem, asem, gsem, row_send, row_recv, slot_send, slot_recv, far_send, far_recv, back_send, back_recv,
):
    hs = n // 2
    rd, width = rows.shape[1], rows.shape[2]
    hid = wbuf.shape[2]
    span = width // PARTS
    lg = lax.axis_index("league")
    rp = lax.axis_index("rep")
    n_rep = lax.axis_size("rep")
    partner = lax.rem(rp + n_rep // 2, n_rep)
    sibling = rp + 1 - 2 * lax.rem(rp, 2)
    half = lg // hs
    pos = lax.rem(lg, hs)
    far_half = 1 - half
    zbit, y = pos // 2, lax.rem(pos, 2)
    inner = jnp.where(half + zbit == 1, 1, 0)
    level = half * hs + (1 - zbit) * 2 + y
    across = lg + 2 - 4 * half
    beside = lg + 1 - 2 * y

    def greet(sem, to):
        pl.semaphore_signal(sem, inc=1, device_id=to, device_id_type=MESH)

    barrier = pltpu.get_barrier_semaphore()

    @pl.when(inner == 1)
    def _():
        greet(barrier, (across, rp))

    for to in ((level, rp), (beside, rp), (lg, partner), (lg, sibling)):
        greet(barrier, to)

    def local(src, dst, which):
        return pltpu.make_async_copy(src, dst, lsem.at[which])

    copy_obs = local(obs_hbm, rows.at[0], 0)
    copy_w = local(w_hbm, wbuf.at[0], 1)
    copy_gain = local(gain_hbm, gain, 2)
    copy_head = local(head_hbm, head, 3)
    copy_pair = local(pair_hbm, pair, 4)
    copy_live = local(valid_hbm, live, 5)
    for move in (copy_pair, copy_live, copy_obs, copy_head, copy_w, copy_gain):
        move.start()

    sub = lax.broadcasted_iota(jnp.int32, (rd, rd), 0)
    lane = lax.broadcasted_iota(jnp.int32, (rd, rd), 1)
    agent_sub = lax.broadcasted_iota(jnp.int32, (n, rd), 0)

    def placing(agent):
        pick = jnp.where(agent == agent_sub, 1.0, 0.0)
        earlier = jnp.where(sub < lane, 1.0, 0.0).astype(jnp.bfloat16)
        before = jnp.dot(pick.astype(jnp.bfloat16), earlier, preferred_element_type=jnp.float32)
        slot = jnp.sum(before * pick, axis=0, keepdims=True).astype(jnp.int32)
        return pick, slot

    def choice(agent, slot, side):
        place = agent * cap + slot - side * rd
        return jnp.where(sub == place, 1.0, 0.0).astype(jnp.bfloat16)

    none = jnp.zeros((cap, width), jnp.bfloat16)
    taken[0, pos] = none
    taken[1, pos] = none
    back[0, lg] = jnp.zeros((1, rd), jnp.float32)
    back[1, lg] = jnp.zeros((1, rd), jnp.float32)
    copy_pair.wait()
    copy_live.wait()
    my_code = jnp.where(live[...] == 1, pair[...], -1)
    code[0] = my_code
    my_pick, my_slot = placing(my_code)
    my_far = choice(my_code, my_slot, far_half)
    my_near = choice(my_code, my_slot, half)
    copy_obs.wait()

    def fill(which, source, chosen, start, length):
        cols = pl.ds(start, length)
        picked = jnp.dot(chosen, rows[source, :, cols], preferred_element_type=jnp.float32)
        slots[which, :, :, cols] = picked.astype(jnp.bfloat16).reshape(hs, cap, length)

    fill(0, 0, my_far, 0, width)
    fill(1, 0, my_near, 0, width)
    copy_head.wait()
    hv[0] = head[...].astype(jnp.float32)

    def remote(src, dst, send, recv, to):
        return pltpu.make_async_remote_copy(
            src_ref=src, dst_ref=dst, send_sem=send, recv_sem=recv,
            device_id=to, device_id_type=MESH,
        )

    def cut(ref, part):
        return ref.at[:, pl.ds(part * span, span)]

    send_code = remote(code.at[0], code.at[1], asem.at[0, 0], asem.at[1, 0], (lg, partner))
    send_head = remote(hv.at[0], hv.at[1], asem.at[0, 1], asem.at[1, 1], (lg, sibling))
    send_w = remote(wbuf.at[0], wbuf.at[1], asem.at[0, 2], asem.at[1, 2], (lg, sibling))
    send_rows = [
        remote(cut(rows.at[0], p), cut(rows.at[1], p), row_send.at[p], row_recv.at[p], (lg, partner))
        for p in range(PARTS)
    ]

    def spot(u, side_y):
        return jnp.where(half == u, 2, 0) + side_y

    ys = (y, 1 - y)

    def far_copy(u, j, part):
        to = spot(u, ys[j])
        return remote(
            cut(slots.at[0, to], part), cut(distant.at[inner, y], part),
            far_send.at[0, u, j, part], far_recv.at[0, inner, y, part], (far_half * hs + to, rp),
        )

    def arrival(u, j, part):
        return remote(
            cut(slots.at[0, 0], part), cut(distant.at[u, ys[j]], part),
            far_send.at[0, 0, 0, part], far_recv.at[0, u, ys[j], part], (far_half * hs + spot(u, ys[j]), rp),
        )

    def forward_copy(u, j, part):
        return remote(
            cut(distant.at[u, ys[j]], part), cut(distant.at[u, 2 + ys[j]], part),
            far_send.at[1, u, j, part], far_recv.at[1, u, ys[j], part], (lg, partner),
        )

    def landing(u, j, part):
        return remote(
            cut(distant.at[u, ys[j]], part), cut(distant.at[u, 2 + ys[j]], part),
            far_send.at[1, u, j, part], far_recv.at[1, u, ys[j], part], (lg, partner),
        )

    near_to = ((zbit * 2 + 1 - y), ((1 - zbit) * 2 + y), ((1 - zbit) * 2 + 1 - y))

    def near_copy(kind, k, part):
        to = near_to[k]
        return remote(
            cut(slots.at[1 + kind, to], part), cut(taken.at[kind, pos], part),
            slot_send.at[kind, k, part], slot_recv.at[kind, k, part], (half * hs + to, rp),
        )

    def near_whole(k):
        to = near_to[k]
        return remote(
            slots.at[1, to], taken.at[0, pos],
            slot_send.at[0, k, 0], slot_recv.at[0, k, 0], (half * hs + to, rp),
        )

    near0 = [near_whole(k) for k in range(3)]
    near2 = [near_copy(1, k, p) for p in range(PARTS) for k in range(3)]
    far = {(u, j, p): far_copy(u, j, p) for u in range(2) for j in range(2) for p in range(PARTS)}
    onward = {(u, j, p): forward_copy(u, j, p) for u in range(2) for j in range(2) for p in range(PARTS)}

    def send_far(u, j):
        for p in range(PARTS):
            far[u, j, p].start()

    pl.semaphore_wait(barrier, 4 + inner)
    greet(gsem.at[0], (level, rp))

    @pl.when(inner == 1)
    def _():
        greet(gsem.at[1], (across, rp))
        send_far(1, 0)

    send_code.start()
    for move in send_rows:
        move.start()
    near0[0].start()
    near0[1].start()
    copy_w.wait()
    send_head.start()
    send_w.start()
    pl.semaphore_wait(gsem.at[0], 1)

    @pl.when(inner == 1)
    def _():
        pl.semaphore_wait(gsem.at[1], 1)
        greet(gsem.at[2], (level, rp))
        greet(gsem.at[2], (across, rp))
        send_far(0, 0)
        send_far(1, 1)

    @pl.when(inner == 0)
    def _():
        send_far(1, 0)

    near0[2].start()
    pl.semaphore_wait(gsem.at[2], 1)

    @pl.when(inner == 1)
    def _():
        greet(gsem.at[3], (level, rp))
        send_far(0, 1)

    @pl.when(inner == 0)
    def _():
        send_far(0, 0)
        send_far(1, 1)
        pl.semaphore_wait(gsem.at[3], 1)
        send_far(0, 1)

    copy_gain.wait()

    def values(block):
        wide = block.astype(jnp.float32)
        squares = jnp.mean(wide * wide, axis=1, keepdims=True)
        scaled[...] = (wide * lax.rsqrt(squares + 1e-06) * gain[...]).astype(jnp.bfloat16)
        acc = jnp.zeros((rd, rd), jnp.float32)
        for j in range(2):
            for col in range(0, hid, TILE):
                v = jnp.dot(scaled[...], wbuf[j, :, pl.ds(col, TILE)], preferred_element_type=jnp.float32)
                part = v / (1.0 + jnp.exp(-v)) * hv[j, :, pl.ds(col, TILE)]
                for c in range(0, TILE, rd):
                    acc = acc + part[:, c:c + rd]
        return jnp.sum(acc.T, axis=0, keepdims=True)

    replies = []

    def reply(line, index, side, link, to):
        move = remote(
            res.at[line], back.at[side, lg], back_send.at[side, index], back_recv.at[side, link], to,
        )
        move.start()
        replies.append(move)

    def forward(u, j):
        for p in range(PARTS):
            arrival(u, j, p).wait_recv()
            onward[u, j, p].start()

    def answer_near(kind):
        res[kind] = values(taken[kind].reshape(rd, width))
        who = rp if kind == 0 else partner
        for k in range(3):
            reply(kind, k, kind, k, (half * hs + near_to[k], who))

    def answer_far(u):
        for j in range(2):
            for p in range(PARTS):
                landing(u, j, p).wait_recv()
        found = values(distant[u].reshape(rd, width))
        res[2 + 2 * u] = found
        res[3 + 2 * u] = pltpu.roll(found, rd // 2, 1)
        for j in range(2):
            to = far_half * hs + spot(u, ys[j])
            link = 3 + 2 * inner + j
            reply(3 + 2 * u, 3 + 2 * u + j, 1, link, (to, partner))
            reply(2 + 2 * u, 3 + 2 * u + j, 0, link, (to, rp))

    send_head.wait_recv()
    send_w.wait_recv()
    mine = values(rows[0])

    send_code.wait_recv()
    other_code = code[1]
    other_near = choice(other_code, placing(other_code)[1], half)
    for p in range(PARTS):
        send_rows[p].wait_recv()
        fill(2, 1, other_near, p * span, span)
        for k in range(3):
            near2[p * 3 + k].start()
        if p == PARTS - 2:
            forward(0, 0)
    vown[0] = values(rows[1])
    send_own = remote(vown.at[0], vown.at[1], asem.at[0, 3], asem.at[1, 3], (lg, partner))
    send_own.start()
    forward(0, 1)
    for move in near0:
        move.wait_recv()
    answer_near(0)
    forward(1, 0)
    for move in near2:
        move.wait_recv()
    answer_near(1)
    answer_far(0)
    forward(1, 1)
    answer_far(1)

    send_own.wait_recv()
    own = mine + vown[1]
    out_ref[0] = own
    for side in range(2):
        for link in range(7):
            remote(
                res.at[0], back.at[side, lg], back_send.at[side, 0], back_recv.at[side, link], (lg, partner),
            ).wait_recv()
    table = jnp.concatenate([back[0, a] + back[1, a] for a in range(n)], axis=0)
    base = jnp.where(my_code // hs == half, pos, y) * cap
    chosen = jnp.where(sub == my_slot + base, 1.0, 0.0)
    found = jnp.dot(table, chosen, preferred_element_type=jnp.float32, precision=lax.Precision.HIGHEST)
    opp = jnp.sum(jnp.where(my_pick > 0.0, found, 0.0), axis=0, keepdims=True)
    out_ref[1] = jnp.where(my_code == lg, own, opp)
    for move in [send_code, send_head, send_w, send_own, *send_rows, *near0, *near2, *far.values(), *onward.values(), *replies]:
        move.wait_send()


def kernel_plan(observations, weights, gains, heads, pairing, valid):
    rd, width = observations.shape
    hid = weights.shape[2]
    n = lax.axis_size("league")
    cap = 2 * rd // n
    hs = n // 2
    vmem = pl.BlockSpec(memory_space=pltpu.VMEM)
    anywhere = pl.BlockSpec(memory_space=pl.ANY)
    both = pl.pallas_call(
        functools.partial(kernel, n, cap),
        out_shape=jax.ShapeDtypeStruct((2, 1, rd), jnp.float32),
        in_specs=[anywhere] * 6,
        out_specs=vmem,
        scratch_shapes=[
            pltpu.VMEM((2, rd, width), jnp.bfloat16),
            pltpu.VMEM((2, width, hid), jnp.bfloat16),
            pltpu.VMEM((1, width), jnp.float32),
            pltpu.VMEM((1, hid), jnp.bfloat16),
            pltpu.VMEM((1, rd), jnp.int32),
            pltpu.VMEM((1, rd), jnp.int32),
            pltpu.VMEM((2, 1, hid), jnp.float32),
            pltpu.VMEM((2, 1, rd), jnp.int32),
            pltpu.VMEM((3, hs, cap, width), jnp.bfloat16),
            pltpu.VMEM((2, hs, cap, width), jnp.bfloat16),
            pltpu.VMEM((2, hs, cap, width), jnp.bfloat16),
            pltpu.VMEM((rd, width), jnp.bfloat16),
            pltpu.VMEM((6, 1, rd), jnp.float32),
            pltpu.VMEM((2, n, 1, rd), jnp.float32),
            pltpu.VMEM((2, 1, rd), jnp.float32),
            pltpu.SemaphoreType.DMA((6,)),
            pltpu.SemaphoreType.DMA((2, 4)),
            pltpu.SemaphoreType.REGULAR((4,)),
            pltpu.SemaphoreType.DMA((PARTS,)),
            pltpu.SemaphoreType.DMA((PARTS,)),
            pltpu.SemaphoreType.DMA((2, 3, PARTS)),
            pltpu.SemaphoreType.DMA((2, 3, PARTS)),
            pltpu.SemaphoreType.DMA((2, 2, 2, PARTS)),
            pltpu.SemaphoreType.DMA((2, 2, 2, PARTS)),
            pltpu.SemaphoreType.DMA((2, 7)),
            pltpu.SemaphoreType.DMA((2, 7)),
        ],
        compiler_params=pltpu.CompilerParams(collective_id=0, has_side_effects=True),
    )(
        observations, weights[0], gains, heads,
        pairing.reshape(1, rd), valid.reshape(1, rd),
    )
    return both[0, 0], both[1, 0]


def per_device(observations, weights, gains, heads, pairing, valid):
    rd = observations.shape[0]
    n = lax.axis_size("league")
    cap = 2 * rd // n
    fits = (
        n == 8 and cap % 16 == 0 and rd == 128
        and lax.axis_size("rep") == 4 and weights.shape[2] % TILE == 0
    )
    plan = kernel_plan if fits else gathered_plan
    return plan(observations, weights, gains, heads, pairing, valid)


def solution(mesh):
    return jax.shard_map(
        per_device,
        mesh=mesh,
        in_specs=(
            P(("league", "rep"), None),
            P("league", None, "rep"),
            P("league", None),
            P("league", "rep"),
            P(("league", "rep"), None),
            P(("league", "rep")),
        ),
        out_specs=(P(("league", "rep")), P(("league", "rep"))),
        check_vma=False,
    )
```

```python
import functools

import jax
import jax.numpy as jnp
from jax import lax
from jax.experimental import pallas as pl
from jax.experimental.pallas import tpu as pltpu
from jax.sharding import PartitionSpec as P

MESH = pl.DeviceIdType.MESH
TILE = 512
PARTS = 4


def normed_values(obs_rows, agent_gain, weight_cols, head_cols):
    wide_rows = obs_rows.astype(jnp.float32)
    squares = jnp.mean(wide_rows * wide_rows, axis=1, keepdims=True)
    scaled = (wide_rows * lax.rsqrt(squares + 1e-06) * agent_gain).astype(jnp.bfloat16)
    hidden = jax.nn.silu(jnp.dot(scaled, weight_cols, preferred_element_type=jnp.float32))
    return jnp.sum(hidden * head_cols.astype(jnp.float32), axis=1)


def gathered_plan(observations, weights, gains, heads, pairing, valid):
    rows_dev, feature_width = observations.shape
    n_league = lax.axis_size("league")
    capacity = max(2, 2 * rows_dev // n_league)
    own_gain = gains[0]
    weight_full = lax.all_gather(weights[0], "rep", axis=1, tiled=True)
    head_full = lax.all_gather(heads[0], "rep", axis=0, tiled=True)
    own_value = normed_values(observations, own_gain, weight_full, head_full)
    owner_id = pairing[:, 0]
    is_live = valid == 1
    agent_iota = jnp.arange(n_league, dtype=jnp.int32)
    pick_table = ((owner_id[:, None] == agent_iota[None, :]) & is_live[:, None]).astype(jnp.float32)
    row_iota = jnp.arange(rows_dev, dtype=jnp.int32)
    earlier = (row_iota[:, None] > row_iota[None, :]).astype(jnp.float32)
    before = jnp.dot(earlier, pick_table, precision=lax.Precision.HIGHEST)
    slot_index = jnp.sum(before * pick_table, axis=1).astype(jnp.int32)
    target = jnp.where(is_live, owner_id * capacity + slot_index, n_league * capacity)
    outgoing = (
        jnp.zeros((n_league * capacity + 1, feature_width), jnp.bfloat16)
        .at[target]
        .set(observations)
    )
    outgoing = outgoing[: n_league * capacity].reshape(n_league, capacity, feature_width)
    received = lax.all_to_all(outgoing, "league", split_axis=0, concat_axis=0, tiled=True)
    flat_rows = received.reshape(received.shape[0] * received.shape[1], feature_width)
    answers = normed_values(flat_rows, own_gain, weight_full, head_full).reshape(
        received.shape[0], received.shape[1]
    )
    returned = lax.all_to_all(answers, "league", split_axis=0, concat_axis=0, tiled=True)
    flat_back = jnp.concatenate([returned.reshape(-1), jnp.zeros((1,), jnp.float32)])
    opponent_value = jnp.where(is_live, flat_back[target], 0.0)
    return (own_value, opponent_value)


def kernel(
    n, cap,
    obs_hbm, w_hbm, gain_hbm, head_hbm, pair_hbm, valid_hbm,
    out_ref,
    rows, wbuf, gain, head, pair, live, hv, code, slots, taken, distant, scaled, res, back, vown,
    lsem, gsem, sent, came, row_came, far_came,
):
    hs = n // 2
    rd, width = rows.shape[1], rows.shape[2]
    hid = wbuf.shape[2]
    span = width // PARTS
    lg = lax.axis_index("league")
    rp = lax.axis_index("rep")
    n_rep = lax.axis_size("rep")
    partner = lax.rem(rp + n_rep // 2, n_rep)
    sibling = rp + 1 - 2 * lax.rem(rp, 2)
    half = lg // hs
    pos = lax.rem(lg, hs)
    far_half = 1 - half
    zbit, y = pos // 2, lax.rem(pos, 2)
    inner = jnp.where(half + zbit == 1, 1, 0)
    level = half * hs + (1 - zbit) * 2 + y
    across = lg + 2 - 4 * half
    beside = lg + 1 - 2 * y

    def greet(sem, to):
        pl.semaphore_signal(sem, inc=1, device_id=to, device_id_type=MESH)

    barrier = pltpu.get_barrier_semaphore()

    @pl.when(inner == 1)
    def _():
        greet(barrier, (across, rp))

    for to in ((level, rp), (beside, rp), (lg, partner), (lg, sibling)):
        greet(barrier, to)

    def local(src, dst, which):
        return pltpu.make_async_copy(src, dst, lsem.at[which])

    copy_obs = local(obs_hbm, rows.at[0], 0)
    copy_w = local(w_hbm, wbuf.at[0], 1)
    copy_gain = local(gain_hbm, gain, 2)
    copy_head = local(head_hbm, head, 3)
    copy_pair = local(pair_hbm, pair, 4)
    copy_live = local(valid_hbm, live, 5)
    for move in (copy_pair, copy_live, copy_obs, copy_head, copy_w, copy_gain):
        move.start()

    sub = lax.broadcasted_iota(jnp.int32, (rd, rd), 0)
    lane = lax.broadcasted_iota(jnp.int32, (rd, rd), 1)
    agent_sub = lax.broadcasted_iota(jnp.int32, (n, rd), 0)

    def placing(agent):
        pick = jnp.where(agent == agent_sub, 1.0, 0.0)
        earlier = jnp.where(sub < lane, 1.0, 0.0).astype(jnp.bfloat16)
        before = jnp.dot(pick.astype(jnp.bfloat16), earlier, preferred_element_type=jnp.float32)
        slot = jnp.sum(before * pick, axis=0, keepdims=True).astype(jnp.int32)
        return pick, slot

    def choice(agent, slot, side):
        place = agent * cap + slot - side * rd
        return jnp.where(sub == place, 1.0, 0.0).astype(jnp.bfloat16)

    none = jnp.zeros((cap, width), jnp.bfloat16)
    taken[0, pos] = none
    taken[1, pos] = none
    back[0, lg] = jnp.zeros((1, rd), jnp.float32)
    back[1, lg] = jnp.zeros((1, rd), jnp.float32)
    copy_pair.wait()
    copy_live.wait()
    my_code = jnp.where(live[...] == 1, pair[...], -1)
    code[0] = my_code
    my_pick, my_slot = placing(my_code)
    my_far = choice(my_code, my_slot, far_half)
    my_near = choice(my_code, my_slot, half)
    copy_obs.wait()

    def fill(which, source, chosen, start, length):
        cols = pl.ds(start, length)
        picked = jnp.dot(chosen, rows[source, :, cols], preferred_element_type=jnp.float32)
        slots[which, :, :, cols] = picked.astype(jnp.bfloat16).reshape(hs, cap, length)

    fill(0, 0, my_far, 0, width)
    fill(1, 0, my_near, 0, width)
    copy_head.wait()
    hv[0] = head[...].astype(jnp.float32)

    def remote(src, dst, send, recv, to):
        return pltpu.make_async_remote_copy(
            src_ref=src, dst_ref=dst, send_sem=send, recv_sem=recv,
            device_id=to, device_id_type=MESH,
        )

    def cut(ref, part):
        return ref.at[:, pl.ds(part * span, span)]

    send_code = remote(code.at[0], code.at[1], sent.at[0], came.at[0], (lg, partner))
    send_head = remote(hv.at[0], hv.at[1], sent.at[1], came.at[1], (lg, sibling))
    send_w = remote(wbuf.at[0], wbuf.at[1], sent.at[2], came.at[2], (lg, sibling))
    send_rows = [
        remote(cut(rows.at[0], p), cut(rows.at[1], p), sent.at[3], row_came.at[p], (lg, partner))
        for p in range(PARTS)
    ]

    def spot(u, side_y):
        return jnp.where(half == u, 2, 0) + side_y

    ys = (y, 1 - y)

    def far_copy(u, j, part):
        to = spot(u, ys[j])
        return remote(
            cut(slots.at[0, to], part), cut(distant.at[inner, y], part),
            sent.at[4], far_came.at[inner, y, part], (far_half * hs + to, rp),
        )

    def arrival(u, j, part):
        return remote(
            cut(slots.at[0, 0], part), cut(distant.at[u, ys[j]], part),
            sent.at[4], far_came.at[u, ys[j], part], (far_half * hs + spot(u, ys[j]), rp),
        )

    def forward_copy(u, j, part):
        return remote(
            cut(distant.at[u, ys[j]], part), cut(distant.at[u, 2 + ys[j]], part),
            sent.at[5], came.at[4 + u], (lg, partner),
        )

    near_to = ((zbit * 2 + 1 - y), ((1 - zbit) * 2 + y), ((1 - zbit) * 2 + 1 - y))

    def near_copy(kind, k, part):
        to = near_to[k]
        return remote(
            cut(slots.at[1 + kind, to], part), cut(taken.at[kind, pos], part),
            sent.at[7], came.at[7], (half * hs + to, rp),
        )

    def near_whole(k):
        to = near_to[k]
        return remote(
            slots.at[1, to], taken.at[0, pos],
            sent.at[6], came.at[6], (half * hs + to, rp),
        )

    def whole(ref, out, into):
        return remote(ref, ref, sent.at[out], came.at[into], (lg, partner))

    near0 = [near_whole(k) for k in range(3)]
    near2 = [near_copy(1, k, p) for p in range(PARTS) for k in range(3)]
    far = {(u, j, p): far_copy(u, j, p) for u in range(2) for j in range(2) for p in range(PARTS)}
    onward = {(u, j, p): forward_copy(u, j, p) for u in range(2) for j in range(2) for p in range(PARTS)}

    def send_far(u, j):
        for p in range(PARTS):
            far[u, j, p].start()

    pl.semaphore_wait(barrier, 4 + inner)
    greet(gsem.at[0], (level, rp))

    @pl.when(inner == 1)
    def _():
        greet(gsem.at[1], (across, rp))
        send_far(1, 0)

    send_code.start()
    for move in send_rows:
        move.start()
    near0[0].start()
    near0[1].start()
    copy_w.wait()
    send_head.start()
    send_w.start()
    pl.semaphore_wait(gsem.at[0], 1)

    @pl.when(inner == 1)
    def _():
        pl.semaphore_wait(gsem.at[1], 1)
        greet(gsem.at[2], (level, rp))
        greet(gsem.at[2], (across, rp))
        send_far(0, 0)

    @pl.when(inner == 0)
    def _():
        send_far(1, 0)

    near0[2].start()
    pl.semaphore_wait(gsem.at[2], 1)

    @pl.when(inner == 1)
    def _():
        greet(gsem.at[3], (level, rp))
        send_far(0, 1)
        send_far(1, 1)

    @pl.when(inner == 0)
    def _():
        send_far(0, 0)
        send_far(1, 1)
        pl.semaphore_wait(gsem.at[3], 1)
        send_far(0, 1)

    copy_gain.wait()

    def values(block):
        wide = block.astype(jnp.float32)
        squares = jnp.mean(wide * wide, axis=1, keepdims=True)
        scaled[...] = (wide * lax.rsqrt(squares + 1e-06) * gain[...]).astype(jnp.bfloat16)
        acc = jnp.zeros((rd, rd), jnp.float32)
        for j in range(2):
            for col in range(0, hid, TILE):
                v = jnp.dot(scaled[...], wbuf[j, :, pl.ds(col, TILE)], preferred_element_type=jnp.float32)
                part = v / (1.0 + jnp.exp(-v)) * hv[j, :, pl.ds(col, TILE)]
                for c in range(0, TILE, rd):
                    acc = acc + part[:, c:c + rd]
        return jnp.sum(acc.T, axis=0, keepdims=True)

    def reply(line, side, to):
        remote(res.at[line], back.at[side, lg], sent.at[0], came.at[8], to).start()

    def forward(u, j, first, last):
        for p in range(first, last):
            arrival(u, j, p).wait_recv()
            onward[u, j, p].start()

    def answer_near(kind):
        res[kind] = values(taken[kind].reshape(rd, width))
        who = rp if kind == 0 else partner
        for k in range(3):
            reply(kind, kind, (half * hs + near_to[k], who))

    def answer_far(u):
        whole(distant.at[u, pl.ds(0, 2)], 5, 4 + u).wait_recv()
        found = values(distant[u].reshape(rd, width))
        res[2 + 2 * u] = found
        res[3 + 2 * u] = pltpu.roll(found, rd // 2, 1)
        for j in range(2):
            to = far_half * hs + spot(u, ys[j])
            reply(3 + 2 * u, 1, (to, partner))
            reply(2 + 2 * u, 0, (to, rp))

    send_head.wait_recv()
    send_w.wait_recv()
    mine = values(rows[0])

    send_code.wait_recv()
    other_code = code[1]
    other_near = choice(other_code, placing(other_code)[1], half)
    for p in range(PARTS):
        send_rows[p].wait_recv()
        fill(2, 1, other_near, p * span, span)
        for k in range(3):
            near2[p * 3 + k].start()
        if p == PARTS - 2:
            forward(1, 0, 0, 2)
            forward(0, 0, 0, PARTS)
    vown[0] = values(rows[1])
    send_own = remote(vown.at[0], vown.at[1], sent.at[0], came.at[3], (lg, partner))
    send_own.start()
    forward(1, 0, 2, PARTS)
    forward(0, 1, 0, PARTS)
    whole(taken.at[0, pl.ds(0, 3)], 6, 6).wait_recv()
    answer_near(0)
    forward(1, 1, 0, PARTS)
    answer_far(0)
    whole(taken.at[1, pl.ds(0, 3)], 7, 7).wait_recv()
    answer_near(1)
    answer_far(1)

    send_own.wait_recv()
    own = mine + vown[1]
    out_ref[0] = own
    whole(back.at[:, pl.ds(0, n - 1)], 0, 8).wait_recv()
    table = jnp.concatenate([back[0, a] + back[1, a] for a in range(n)], axis=0)
    base = jnp.where(my_code // hs == half, pos, y) * cap
    chosen = jnp.where(sub == my_slot + base, 1.0, 0.0)
    found = jnp.dot(table, chosen, preferred_element_type=jnp.float32, precision=lax.Precision.HIGHEST)
    opp = jnp.sum(jnp.where(my_pick > 0.0, found, 0.0), axis=0, keepdims=True)
    out_ref[1] = jnp.where(my_code == lg, own, opp)
    for ref, out in (
        (back, 0), (hv.at[0], 1), (wbuf.at[0], 2), (rows.at[0], 3), (slots.at[0], 4), (slots.at[0], 5),
        (slots.at[1, pl.ds(0, 3)], 6), (slots.at[2, pl.ds(0, 3)], 7),
    ):
        whole(ref, out, 0).wait_send()


def kernel_plan(observations, weights, gains, heads, pairing, valid):
    rd, width = observations.shape
    hid = weights.shape[2]
    n = lax.axis_size("league")
    cap = 2 * rd // n
    hs = n // 2
    vmem = pl.BlockSpec(memory_space=pltpu.VMEM)
    anywhere = pl.BlockSpec(memory_space=pl.ANY)
    both = pl.pallas_call(
        functools.partial(kernel, n, cap),
        out_shape=jax.ShapeDtypeStruct((2, 1, rd), jnp.float32),
        in_specs=[anywhere] * 6,
        out_specs=vmem,
        scratch_shapes=[
            pltpu.VMEM((2, rd, width), jnp.bfloat16),
            pltpu.VMEM((2, width, hid), jnp.bfloat16),
            pltpu.VMEM((1, width), jnp.float32),
            pltpu.VMEM((1, hid), jnp.bfloat16),
            pltpu.VMEM((1, rd), jnp.int32),
            pltpu.VMEM((1, rd), jnp.int32),
            pltpu.VMEM((2, 1, hid), jnp.float32),
            pltpu.VMEM((2, 1, rd), jnp.int32),
            pltpu.VMEM((3, hs, cap, width), jnp.bfloat16),
            pltpu.VMEM((2, hs, cap, width), jnp.bfloat16),
            pltpu.VMEM((2, hs, cap, width), jnp.bfloat16),
            pltpu.VMEM((rd, width), jnp.bfloat16),
            pltpu.VMEM((6, 1, rd), jnp.float32),
            pltpu.VMEM((2, n, 1, rd), jnp.float32),
            pltpu.VMEM((2, 1, rd), jnp.float32),
            pltpu.SemaphoreType.DMA((6,)),
            pltpu.SemaphoreType.REGULAR((4,)),
            pltpu.SemaphoreType.DMA((8,)),
            pltpu.SemaphoreType.DMA((9,)),
            pltpu.SemaphoreType.DMA((PARTS,)),
            pltpu.SemaphoreType.DMA((2, 2, PARTS)),
        ],
        compiler_params=pltpu.CompilerParams(collective_id=0, has_side_effects=True),
    )(
        observations, weights[0], gains, heads,
        pairing.reshape(1, rd), valid.reshape(1, rd),
    )
    return both[0, 0], both[1, 0]


def per_device(observations, weights, gains, heads, pairing, valid):
    rd = observations.shape[0]
    n = lax.axis_size("league")
    cap = 2 * rd // n
    fits = (
        n == 8 and cap % 16 == 0 and rd == 128
        and lax.axis_size("rep") == 4 and weights.shape[2] % TILE == 0
    )
    plan = kernel_plan if fits else gathered_plan
    return plan(observations, weights, gains, heads, pairing, valid)


def solution(mesh):
    return jax.shard_map(
        per_device,
        mesh=mesh,
        in_specs=(
            P(("league", "rep"), None),
            P("league", None, "rep"),
            P("league", None),
            P("league", "rep"),
            P(("league", "rep"), None),
            P(("league", "rep")),
        ),
        out_specs=(P(("league", "rep")), P(("league", "rep"))),
        check_vma=False,
    )
```
